32 devices in a mesh: dp: 2 (over z, core), tp: 16 (over x, y).
Axes of the slice: x: 4, y: 4, z: 1, core: 2. Of those that a mesh axis runs over, the one named last changes fastest.
The devices are a block of a 4x4x8 slice.
Arguments:
- x: bfloat16 [4096, 7168], P('dp'), parts along dimension 0
- w_gate: bfloat16 [7168, 20480], P(None, 'tp')
- w_up: bfloat16 [7168, 20480], P(None, 'tp')
- w_down: bfloat16 [20480, 7168], P('tp')
Outputs:
- output: bfloat16 [4096, 7168], P('dp'), parts along dimension 0
There are 2 independent parts. The reference program is written for one: setup_inputs(seed, part) draws one part's arguments, and reference() takes and returns one part's arrays. A program takes and returns all parts, laid end to end along the dimension named above; an argument that names none is the same for every part.
All inputs are finite; a program needn't handle non-finite values.
Results may differ from the reference program's by a relative error of at most 0.016.
Values are sent between devices in bfloat16 or wider.
A program may use at most 768 MiB of HBM per device.

```python
import jax
import jax.numpy as jnp

ROWS = 2048
D = 7168
FF = 20480


def setup_inputs(seed: int = 0, part: int = 0) -> dict:
    kx, kg, ku, kd = jax.random.split(jax.random.key(seed), 4)
    drawn = {
        "x": jax.random.normal(jax.random.fold_in(kx, part), (ROWS, D), jnp.float32),
        "w_gate": jax.random.normal(kg, (D, FF), jnp.float32) * D**-0.5,
        "w_up": jax.random.normal(ku, (D, FF), jnp.float32) * D**-0.5,
        "w_down": jax.random.normal(kd, (FF, D), jnp.float32) * FF**-0.5,
    }
    return {k: v.astype(jnp.bfloat16) for k, v in drawn.items()}


def reference(x, w_gate, w_up, w_down):
    gate = jnp.dot(x, w_gate, preferred_element_type=jnp.float32)
    up = jnp.dot(x, w_up, preferred_element_type=jnp.float32)
    hidden = (jax.nn.silu(gate) * up).astype(jnp.bfloat16)
    return jnp.dot(hidden, w_down, preferred_element_type=jnp.float32).astype(jnp.bfloat16)
```

```python
import functools
import math

import jax
import jax.numpy as jnp
from jax import lax
from jax.experimental import pallas as pl
from jax.experimental.pallas import tpu as pltpu
from jax.sharding import PartitionSpec as P

MESH = pl.DeviceIdType.MESH
COLOURS = 4
CHUNK = 256
TILE = 256
R1, R2, R3, Q1, Q2, Q3, G1, G2, G3, H1, H2, H3 = range(12)


def kernel(cfg, x_hbm, wg_hbm, wu_hbm, wd_hbm, y_hbm,
           xb, wgb, wub, wdb, hb, term, r1, r2, r3, c3, run, s1, s2, q1, q2, q3, cq, fin,
           x_sem, wg_sem, wu_sem, wd_sem, own_sem, send_sem, recv_sem, credit):
    side, chunks, m, q, tiles, tile = cfg
    block, sub = m // side, m // (side * side)
    me = lax.axis_index("tp")
    px, py = me // side, me % side

    def dev(index):
        return {"tp": index}

    def place(k):
        ax = k // 2
        sign = 1 - 2 * (k % 2)
        p1, p2 = px * (1 - ax) + py * ax, py * (1 - ax) + px * ax
        return p1, p2, side * (1 - ax) + ax, (1 - ax) + side * ax, sign

    def step_on(p, stride, delta):
        return me + ((p + delta + side) % side - p) * stride

    def wrap(p, delta):
        return (p + delta + side) % side

    neighbours = [step_on(px, side, 1), step_on(px, side, -1), step_on(py, 1, 1), step_on(py, 1, -1)]
    barrier = pltpu.get_barrier_semaphore()
    for other in neighbours:
        pl.semaphore_signal(barrier, inc=1, device_id=dev(other), device_id_type=MESH)
    pl.semaphore_wait(barrier, len(neighbours))

    def remote(kind, c, k, src, dst, to):
        return pltpu.make_async_remote_copy(
            src_ref=src, dst_ref=dst, send_sem=send_sem.at[kind, c % 2, k],
            recv_sem=recv_sem.at[kind, c % 2, k], device_id=dev(to), device_id_type=MESH)

    def rows_of(start, count):
        return pl.ds(pl.multiple_of(start, count), count)

    def y_at(c, k, p1, p2, count):
        return y_hbm.at[rows_of(c * m + p1 * block + p2 * sub, count), pl.ds(pl.multiple_of(k * q, 128), q)]

    def message(kind, c, k):
        p1, p2, st1, st2, s = place(k)
        par = c % 2
        plus1, minus1 = step_on(p1, st1, s), step_on(p1, st1, -s)
        plus2, minus2 = step_on(p2, st2, s), step_on(p2, st2, -s)
        if kind == R1:
            return remote(kind, c, k, term.at[par, k, rows_of(wrap(p1, 2) * block, block)], r1.at[par, k], minus1)
        if kind == R2:
            return remote(kind, c, k, term.at[par, k, rows_of(wrap(p1, s) * block, block)], r2.at[par, k], plus1)
        if kind == R3:
            return remote(kind, c, k, c3.at[par, k], r3.at[par, k], minus1)
        if kind == Q1:
            return remote(kind, c, k, s1.at[par, k], q1.at[par, k], minus2)
        if kind == Q2:
            return remote(kind, c, k, s2.at[par, k], q2.at[par, k], plus2)
        if kind == Q3:
            return remote(kind, c, k, cq.at[par, k], q3.at[par, k], minus2)
        if kind == G1:
            return remote(kind, c, k, fin.at[par, k], y_at(c, k, p1, p2, sub), plus2)
        if kind == G2:
            return remote(kind, c, k, fin.at[par, k], y_at(c, k, p1, p2, sub), minus2)
        if kind == G3:
            at = y_at(c, k, p1, wrap(p2, -s), sub)
            return remote(kind, c, k, at, at, plus2)
        if kind == H1:
            at = y_at(c, k, p1, 0, block)
            return remote(kind, c, k, at, at, plus1)
        if kind == H2:
            at = y_at(c, k, p1, 0, block)
            return remote(kind, c, k, at, at, minus1)
        at = y_at(c, k, wrap(p1, -s), 0, block)
        return remote(kind, c, k, at, at, plus1)

    def arrived(kind, c, k):
        p1, p2, _, _, s = place(k)
        par = c % 2
        dst = {
            R1: lambda: r1.at[par, k], R2: lambda: r2.at[par, k], R3: lambda: r3.at[par, k],
            Q1: lambda: q1.at[par, k], Q2: lambda: q2.at[par, k], Q3: lambda: q3.at[par, k],
            G1: lambda: y_at(c, k, p1, wrap(p2, -s), sub),
            G2: lambda: y_at(c, k, p1, wrap(p2, s), sub),
            G3: lambda: y_at(c, k, p1, wrap(p2, 2), sub),
            H1: lambda: y_at(c, k, wrap(p1, -s), 0, block),
            H2: lambda: y_at(c, k, wrap(p1, s), 0, block),
            H3: lambda: y_at(c, k, wrap(p1, 2), 0, block),
        }[kind]()
        pltpu.make_async_copy(dst, dst, recv_sem.at[kind, c % 2, k]).wait()

    def own_copy(c, k):
        p1, p2, _, _, _ = place(k)
        return pltpu.make_async_copy(fin.at[c % 2, k], y_at(c, k, p1, p2, sub), own_sem.at[c % 2, k])

    def colours(body):
        def one(k, carry):
            body(k, *place(k))
            return carry
        lax.fori_loop(0, COLOURS, one, 0)

    def by_rows(body):
        def one(i, carry):
            body(pl.multiple_of(i * sub, sub))
            return carry
        lax.fori_loop(0, side, one, 0)

    f32 = jnp.float32

    def stage1(c):
        par, sl = c % 2, c % 3

        def body(k, p1, p2, st1, st2, s):
            message(R1, c, k).wait_send()
            message(R2, c, k).wait_send()
            arrived(R1, c, k)

            def add(i):
                at = pl.ds(i, sub)
                t = term[par, k, pl.ds(pl.multiple_of(wrap(p1, -s) * block + i, sub), sub), :]
                c3[par, k, at, :] = (t.astype(f32) + r1[par, k, at, :].astype(f32)).astype(jnp.bfloat16)
            by_rows(add)
            message(R3, c, k).start()
            arrived(R2, c, k)

            def keep(i):
                at = pl.ds(i, sub)
                t = term[par, k, pl.ds(pl.multiple_of(p1 * block + i, sub), sub), :]
                run[sl, k, at, :] = t.astype(f32) + r2[par, k, at, :].astype(f32)
            by_rows(keep)
        colours(body)

    def stage2(c):
        par, sl = c % 2, c % 3

        def body(k, p1, p2, st1, st2, s):
            message(R3, c, k).wait_send()
            arrived(R3, c, k)

            def add(i):
                at = pl.ds(i, sub)
                run[sl, k, at, :] = run[sl, k, at, :] + r3[par, k, at, :].astype(f32)
            by_rows(add)
            s1[par, k] = run[sl, k, rows_of(wrap(p2, 2) * sub, sub), :].astype(jnp.bfloat16)
            s2[par, k] = run[sl, k, rows_of(wrap(p2, s) * sub, sub), :].astype(jnp.bfloat16)
            message(Q1, c, k).start()
            message(Q2, c, k).start()
        colours(body)

    def stage3(c):
        par, sl = c % 2, c % 3

        def body(k, p1, p2, st1, st2, s):
            message(Q1, c, k).wait_send()
            message(Q2, c, k).wait_send()
            arrived(Q1, c, k)
            there = run[sl, k, rows_of(wrap(p2, -s) * sub, sub), :]
            cq[par, k] = (there + q1[par, k].astype(f32)).astype(jnp.bfloat16)
            message(Q3, c, k).start()
            arrived(Q2, c, k)
            mine = rows_of(p2 * sub, sub)
            run[sl, k, mine, :] = run[sl, k, mine, :] + q2[par, k].astype(f32)
        colours(body)

    def stage4(c):
        par, sl = c % 2, c % 3

        def body(k, p1, p2, st1, st2, s):
            message(Q3, c, k).wait_send()
            arrived(Q3, c, k)
            mine = rows_of(p2 * sub, sub)
            fin[par, k] = (run[sl, k, mine, :] + q3[par, k].astype(f32)).astype(jnp.bfloat16)
            message(G1, c, k).start()
            message(G2, c, k).start()
            own_copy(c, k).start()
        colours(body)

    def stage5(c):
        def body(k, *_):
            message(G1, c, k).wait_send()
            message(G2, c, k).wait_send()
            own_copy(c, k).wait()
            arrived(G1, c, k)
            message(G3, c, k).start()
            arrived(G2, c, k)
        colours(body)

    def stage6(c):
        def body(k, *_):
            message(G3, c, k).wait_send()
            arrived(G3, c, k)
            message(H1, c, k).start()
            message(H2, c, k).start()
        colours(body)

    def stage7(c):
        def body(k, *_):
            message(H1, c, k).wait_send()
            message(H2, c, k).wait_send()
            arrived(H1, c, k)
            message(H3, c, k).start()
            arrived(H2, c, k)
        colours(body)

    def stage8(c):
        def body(k, *_):
            message(H3, c, k).wait_send()
            arrived(H3, c, k)
        colours(body)

    def x_copy(t):
        return pltpu.make_async_copy(x_hbm.at[rows_of(t * m, m), :], xb, x_sem)

    def w_copies(g):
        at = pl.ds(pl.multiple_of((g % tiles) * tile, tile), tile)
        slot = g % 2
        return (pltpu.make_async_copy(wg_hbm.at[:, at], wgb.at[slot], wg_sem.at[slot]),
                pltpu.make_async_copy(wu_hbm.at[:, at], wub.at[slot], wu_sem.at[slot]))

    def colour_at(j):
        return (j % 2) * 2 + j // 2

    def d_copy(j):
        at = pl.ds(pl.multiple_of(colour_at(j) * q, 128), q)
        return pltpu.make_async_copy(wd_hbm.at[:, at], wdb.at[j % 2], wd_sem.at[j % 2])

    x_copy(0).start()
    for g in range(2):
        for copy in w_copies(g):
            copy.start()
    for j in range(2):
        d_copy(j).start()

    def hidden(t):
        x_copy(t).wait()

        def one(n, carry):
            g = t * tiles + n
            slot = g % 2
            for copy in w_copies(g):
                copy.wait()
            gate = jnp.dot(xb[...], wgb[slot], preferred_element_type=f32)
            up = jnp.dot(xb[...], wub[slot], preferred_element_type=f32)
            at = pl.ds(pl.multiple_of(n * tile, tile), tile)
            hb[:, at] = (gate * jax.nn.sigmoid(gate) * up).astype(jnp.bfloat16)

            @pl.when(g + 2 < chunks * tiles)
            def _():
                for copy in w_copies(g + 2):
                    copy.start()
            return carry
        lax.fori_loop(0, tiles, one, 0)

        @pl.when(t + 1 < chunks)
        def _():
            x_copy(t + 1).start()

    def down(t):
        def one(j, carry):
            k = colour_at(j)
            d_copy(j).wait()
            term[t % 2, k] = jnp.dot(hb[...], wdb[j % 2], preferred_element_type=f32).astype(jnp.bfloat16)

            @pl.when((j + 2 < COLOURS) | (t + 1 < chunks))
            def _():
                d_copy((j + 2) % COLOURS).start()
            message(R1, t, k).start()
            message(R2, t, k).start()
            return carry
        lax.fori_loop(0, COLOURS, one, 0)

    late = (stage8, stage7, stage6, stage5, stage4, stage3, stage2)
    steps = chunks + 8

    def step(t, carry):
        @pl.when(t > 0)
        def _():
            for d in range(len(neighbours)):
                pl.semaphore_wait(credit.at[d], 1)

        for i, stage in enumerate(late):
            lag = 8 - i

            @pl.when((t >= lag) & (t < chunks + lag))
            def _(stage=stage, lag=lag):
                stage(t - lag)

        @pl.when(t < chunks)
        def _():
            hidden(t)

        @pl.when((t >= 1) & (t < chunks + 1))
        def _():
            stage1(t - 1)

        @pl.when(t < steps - 1)
        def _():
            for d, other in enumerate(neighbours):
                pl.semaphore_signal(credit.at[d], inc=1, device_id=dev(other), device_id_type=MESH)

        @pl.when(t < chunks)
        def _():
            down(t)
        return carry

    lax.fori_loop(0, steps, step, 0)


def solution(mesh):
    side = math.isqrt(mesh.shape["tp"])
    assert side == 4 and side * side == mesh.shape["tp"]

    def body(x, w_gate, w_up, w_down):
        rows, d = x.shape
        ff = w_gate.shape[1]
        m, q, tile = CHUNK, d // COLOURS, TILE
        chunks, tiles = rows // m, ff // tile
        block, sub = m // side, m // (side * side)
        bf16 = jnp.bfloat16
        any_spec = pl.BlockSpec(memory_space=pl.ANY)
        dma = pltpu.SemaphoreType.DMA
        big = pltpu.VMEM((2, COLOURS, block, q), bf16)
        small = pltpu.VMEM((2, COLOURS, sub, q), bf16)
        return pl.pallas_call(
            functools.partial(kernel, (side, chunks, m, q, tiles, tile)),
            out_shape=jax.ShapeDtypeStruct((rows, d), bf16),
            in_specs=[any_spec] * 4,
            out_specs=any_spec,
            scratch_shapes=[
                pltpu.VMEM((m, d), bf16),
                pltpu.VMEM((2, d, tile), bf16), pltpu.VMEM((2, d, tile), bf16),
                pltpu.VMEM((2, ff, q), bf16),
                pltpu.VMEM((m, ff), bf16),
                pltpu.VMEM((2, COLOURS, m, q), bf16),
                big, big, big, big,
                pltpu.VMEM((3, COLOURS, block, q), jnp.float32),
                small, small, small, small, small, small, small,
                dma, dma((2,)), dma((2,)), dma((2,)), dma((2, COLOURS)),
                dma((12, 2, COLOURS)), dma((12, 2, COLOURS)),
                pltpu.SemaphoreType.REGULAR((4,)),
            ],
            compiler_params=pltpu.CompilerParams(
                collective_id=0, has_side_effects=True, vmem_limit_bytes=66_000_000),
        )(x, w_gate, w_up, w_down)

    return jax.shard_map(
        body,
        mesh=mesh,
        in_specs=(P("dp", None), P(None, "tp"), P(None, "tp"), P("tp", None)),
        out_specs=P("dp", None),
        check_vma=False,
    )
```

```python
import functools
import math

import jax
import jax.numpy as jnp
from jax import lax
from jax.experimental import pallas as pl
from jax.experimental.pallas import tpu as pltpu
from jax.sharding import PartitionSpec as P

MESH = pl.DeviceIdType.MESH
COLOURS = 4
CHUNK = 256
TILE = 256
SLOTS = 3
R1, R2, R3, Q1, Q2, Q3, G1, G2, G3, H1, H2, H3 = range(12)


def kernel(cfg, x_hbm, wg_hbm, wu_hbm, wd_hbm, y_hbm,
           xb, wb, wdb, hb, term, r1, r2, r3, c3, run, s1, s2, q1, q2, q3, cq, fin,
           x_sem, wg_sem, wu_sem, wd_sem, own_sem, send_sem, recv_sem, credit):
    side, chunks, m, q, tiles, tile = cfg
    block, sub = m // side, m // (side * side)
    me = lax.axis_index("tp")
    px, py = me // side, me % side

    def dev(index):
        return {"tp": index}

    def place(k):
        ax = k // 2
        sign = 1 - 2 * (k % 2)
        p1, p2 = px * (1 - ax) + py * ax, py * (1 - ax) + px * ax
        return p1, p2, side * (1 - ax) + ax, (1 - ax) + side * ax, sign

    def step_on(p, stride, delta):
        return me + ((p + delta + side) % side - p) * stride

    def wrap(p, delta):
        return (p + delta + side) % side

    neighbours = [step_on(px, side, 1), step_on(px, side, -1), step_on(py, 1, 1), step_on(py, 1, -1)]
    barrier = pltpu.get_barrier_semaphore()
    for other in neighbours:
        pl.semaphore_signal(barrier, inc=1, device_id=dev(other), device_id_type=MESH)
    pl.semaphore_wait(barrier, len(neighbours))

    def remote(kind, c, k, src, dst, to):
        return pltpu.make_async_remote_copy(
            src_ref=src, dst_ref=dst, send_sem=send_sem.at[kind, c % 2, k],
            recv_sem=recv_sem.at[kind, c % 2, k], device_id=dev(to), device_id_type=MESH)

    def rows_of(start, count):
        return pl.ds(pl.multiple_of(start, count), count)

    def y_at(c, k, p1, p2, count):
        return y_hbm.at[rows_of(c * m + p1 * block + p2 * sub, count), pl.ds(pl.multiple_of(k * q, 128), q)]

    def message(kind, c, k):
        p1, p2, st1, st2, s = place(k)
        par = c % 2
        plus1, minus1 = step_on(p1, st1, s), step_on(p1, st1, -s)
        plus2, minus2 = step_on(p2, st2, s), step_on(p2, st2, -s)
        if kind == R1:
            return remote(kind, c, k, term.at[par, k, rows_of(wrap(p1, 2) * block, block)], r1.at[par, k], minus1)
        if kind == R2:
            return remote(kind, c, k, term.at[par, k, rows_of(wrap(p1, s) * block, block)], r2.at[par, k], plus1)
        if kind == R3:
            return remote(kind, c, k, c3.at[par, k], r3.at[par, k], minus1)
        if kind == Q1:
            return remote(kind, c, k, s1.at[par, k], q1.at[par, k], minus2)
        if kind == Q2:
            return remote(kind, c, k, s2.at[par, k], q2.at[par, k], plus2)
        if kind == Q3:
            return remote(kind, c, k, cq.at[par, k], q3.at[par, k], minus2)
        if kind == G1:
            return remote(kind, c, k, fin.at[par, k], y_at(c, k, p1, p2, sub), plus2)
        if kind == G2:
            return remote(kind, c, k, fin.at[par, k], y_at(c, k, p1, p2, sub), minus2)
        if kind == G3:
            at = y_at(c, k, p1, wrap(p2, -s), sub)
            return remote(kind, c, k, at, at, plus2)
        if kind == H1:
            at = y_at(c, k, p1, 0, block)
            return remote(kind, c, k, at, at, plus1)
        if kind == H2:
            at = y_at(c, k, p1, 0, block)
            return remote(kind, c, k, at, at, minus1)
        at = y_at(c, k, wrap(p1, -s), 0, block)
        return remote(kind, c, k, at, at, plus1)

    def arrived(kind, c, k):
        p1, p2, _, _, s = place(k)
        par = c % 2
        dst = {
            R1: lambda: r1.at[par, k], R2: lambda: r2.at[par, k], R3: lambda: r3.at[par, k],
            Q1: lambda: q1.at[par, k], Q2: lambda: q2.at[par, k], Q3: lambda: q3.at[par, k],
            G1: lambda: y_at(c, k, p1, wrap(p2, -s), sub),
            G2: lambda: y_at(c, k, p1, wrap(p2, s), sub),
            G3: lambda: y_at(c, k, p1, wrap(p2, 2), sub),
            H1: lambda: y_at(c, k, wrap(p1, -s), 0, block),
            H2: lambda: y_at(c, k, wrap(p1, s), 0, block),
            H3: lambda: y_at(c, k, wrap(p1, 2), 0, block),
        }[kind]()
        pltpu.make_async_copy(dst, dst, recv_sem.at[kind, c % 2, k]).wait()

    def own_copy(c, k):
        p1, p2, _, _, _ = place(k)
        return pltpu.make_async_copy(fin.at[c % 2, k], y_at(c, k, p1, p2, sub), own_sem.at[c % 2, k])

    def colours(body):
        def one(k, carry):
            body(k, *place(k))
            return carry
        lax.fori_loop(0, COLOURS, one, 0)

    def by_rows(body):
        def one(i, carry):
            body(pl.multiple_of(i * sub, sub))
            return carry
        lax.fori_loop(0, side, one, 0)

    f32 = jnp.float32

    def stage1(c):
        par = c % 2

        def pass_on(k, p1, p2, st1, st2, s):
            message(R1, c, k).wait_send()
            arrived(R1, c, k)

            def add(i):
                at = pl.ds(i, sub)
                t = term[par, k, pl.ds(pl.multiple_of(wrap(p1, -s) * block + i, sub), sub), :]
                c3[par, k, at, :] = (t.astype(f32) + r1[par, k, at, :].astype(f32)).astype(jnp.bfloat16)
            by_rows(add)
            message(R3, c, k).start()

        def keep(k, p1, p2, st1, st2, s):
            message(R2, c, k).wait_send()
            arrived(R2, c, k)

            def add(i):
                at = pl.ds(i, sub)
                t = term[par, k, pl.ds(pl.multiple_of(p1 * block + i, sub), sub), :]
                run[par, k, at, :] = t.astype(f32) + r2[par, k, at, :].astype(f32)
            by_rows(add)
        colours(pass_on)
        colours(keep)

    def stage2(c):
        par = c % 2

        def body(k, p1, p2, st1, st2, s):
            message(R3, c, k).wait_send()
            arrived(R3, c, k)

            def add(i):
                at = pl.ds(i, sub)
                run[par, k, at, :] = run[par, k, at, :] + r3[par, k, at, :].astype(f32)
            by_rows(add)
            s1[par, k] = run[par, k, rows_of(wrap(p2, 2) * sub, sub), :].astype(jnp.bfloat16)
            s2[par, k] = run[par, k, rows_of(wrap(p2, s) * sub, sub), :].astype(jnp.bfloat16)
            message(Q1, c, k).start()
            message(Q2, c, k).start()
        colours(body)

    def stage3(c):
        par = c % 2

        def pass_on(k, p1, p2, st1, st2, s):
            message(Q1, c, k).wait_send()
            arrived(Q1, c, k)
            there = run[par, k, rows_of(wrap(p2, -s) * sub, sub), :]
            cq[par, k] = (there + q1[par, k].astype(f32)).astype(jnp.bfloat16)
            message(Q3, c, k).start()

        def keep(k, p1, p2, st1, st2, s):
            message(Q2, c, k).wait_send()
            arrived(Q2, c, k)
            mine = rows_of(p2 * sub, sub)
            run[par, k, mine, :] = run[par, k, mine, :] + q2[par, k].astype(f32)
        colours(pass_on)
        colours(keep)

    def stage4(c):
        par = c % 2

        def body(k, p1, p2, st1, st2, s):
            message(Q3, c, k).wait_send()
            arrived(Q3, c, k)
            mine = rows_of(p2 * sub, sub)
            fin[par, k] = (run[par, k, mine, :] + q3[par, k].astype(f32)).astype(jnp.bfloat16)
            message(G1, c, k).start()
            own_copy(c, k).start()
        colours(body)
        colours(lambda k, *_: message(G2, c, k).start())

    def stage5(c):
        def pass_on(k, *_):
            message(G1, c, k).wait_send()
            arrived(G1, c, k)
            message(G3, c, k).start()

        def rest(k, *_):
            message(G2, c, k).wait_send()
            own_copy(c, k).wait()
            arrived(G2, c, k)
        colours(pass_on)
        colours(rest)

    def stage6(c):
        def body(k, *_):
            message(G3, c, k).wait_send()
            arrived(G3, c, k)
            message(H1, c, k).start()
        colours(body)
        colours(lambda k, *_: message(H2, c, k).start())

    def stage7(c):
        def pass_on(k, *_):
            message(H1, c, k).wait_send()
            arrived(H1, c, k)
            message(H3, c, k).start()

        def rest(k, *_):
            message(H2, c, k).wait_send()
            arrived(H2, c, k)
        colours(pass_on)
        colours(rest)

    def stage8(c):
        def body(k, *_):
            message(H3, c, k).wait_send()
            arrived(H3, c, k)
        colours(body)

    def x_copy(t):
        return pltpu.make_async_copy(x_hbm.at[rows_of(t * m, m), :], xb, x_sem)

    def w_copies(g):
        at = pl.ds(pl.multiple_of((g % tiles) * tile, tile), tile)
        slot = g % SLOTS
        return (pltpu.make_async_copy(wg_hbm.at[:, at], wb.at[slot, :, pl.ds(0, tile)], wg_sem.at[slot]),
                pltpu.make_async_copy(wu_hbm.at[:, at], wb.at[slot, :, pl.ds(tile, tile)], wu_sem.at[slot]))

    def colour_at(j):
        return (j % 2) * 2 + j // 2

    def d_copy(j):
        at = pl.ds(pl.multiple_of(colour_at(j) * q, 128), q)
        return pltpu.make_async_copy(wd_hbm.at[:, at], wdb.at[j % 2], wd_sem.at[j % 2])

    x_copy(0).start()
    for g in range(SLOTS):
        for copy in w_copies(g):
            copy.start()

    def hidden(t, n):
        @pl.when(n == 0)
        def _():
            x_copy(t).wait()
        g = t * tiles + n
        slot = g % SLOTS
        for copy in w_copies(g):
            copy.wait()
        both = jnp.dot(xb[...], wb[slot], preferred_element_type=f32)
        gate, up = both[:, :tile], both[:, tile:]
        at = pl.ds(pl.multiple_of(n * tile, tile), tile)
        hb[:, at] = (gate * jax.nn.sigmoid(gate) * up).astype(jnp.bfloat16)

        @pl.when(g + SLOTS < chunks * tiles)
        def _():
            for copy in w_copies(g + SLOTS):
                copy.start()

        @pl.when((t == 0) & (n >= tiles - 2))
        def _():
            d_copy(n - (tiles - 2)).start()

        @pl.when((n == tiles - 1) & (t + 1 < chunks))
        def _():
            x_copy(t + 1).start()

    def down(t, j):
        k = colour_at(j)
        d_copy(j).wait()
        term[t % 2, k] = jnp.dot(hb[...], wdb[j % 2], preferred_element_type=f32).astype(jnp.bfloat16)
        message(R1, t, k).start()
        message(R2, t, k).start()

        @pl.when((j + 2 < COLOURS) | (t + 1 < chunks))
        def _():
            d_copy((j + 2) % COLOURS).start()

    steps = chunks + 6

    def handle(t, *stages):
        for lag, stage in stages:
            @pl.when((t >= lag) & (t < chunks + lag))
            def _(stage=stage, lag=lag):
                stage(t - lag)

    def at_tile(n, late):
        return n == max(tiles - 1 - late, 0)

    def step(t, carry):
        @pl.when(t > 0)
        def _():
            for d in range(len(neighbours)):
                pl.semaphore_wait(credit.at[d], 1)

        handle(t, (5, stage7))

        def tile_step(n, carry):
            @pl.when(t < chunks)
            def _():
                hidden(t, n)

            @pl.when(at_tile(n, 4))
            def _():
                handle(t, (6, stage8), (3, stage5))

            @pl.when(at_tile(n, 2))
            def _():
                handle(t, (2, stage3))

            @pl.when(at_tile(n, 1))
            def _():
                handle(t, (4, stage6), (1, stage1))
            return carry
        lax.fori_loop(0, tiles, tile_step, 0)

        @pl.when(t < steps - 1)
        def _():
            for d, other in enumerate(neighbours):
                pl.semaphore_signal(credit.at[d], inc=1, device_id=dev(other), device_id_type=MESH)

        def colour_step(j, carry):
            @pl.when(j == 1)
            def _():
                handle(t, (2, stage4))

            @pl.when(j == 2)
            def _():
                handle(t, (1, stage2))

            @pl.when(t < chunks)
            def _():
                down(t, j)
            return carry
        lax.fori_loop(0, COLOURS, colour_step, 0)
        return carry

    lax.fori_loop(0, steps, step, 0)


def solution(mesh):
    side = math.isqrt(mesh.shape["tp"])
    assert side == 4 and side * side == mesh.shape["tp"]

    def body(x, w_gate, w_up, w_down):
        rows, d = x.shape
        ff = w_gate.shape[1]
        m, q, tile = CHUNK, d // COLOURS, TILE
        chunks, tiles = rows // m, ff // tile
        block, sub = m // side, m // (side * side)
        bf16 = jnp.bfloat16
        any_spec = pl.BlockSpec(memory_space=pl.ANY)
        dma = pltpu.SemaphoreType.DMA
        big = pltpu.VMEM((2, COLOURS, block, q), bf16)
        small = pltpu.VMEM((2, COLOURS, sub, q), bf16)
        return pl.pallas_call(
            functools.partial(kernel, (side, chunks, m, q, tiles, tile)),
            out_shape=jax.ShapeDtypeStruct((rows, d), bf16),
            in_specs=[any_spec] * 4,
            out_specs=any_spec,
            scratch_shapes=[
                pltpu.VMEM((m, d), bf16),
                pltpu.VMEM((SLOTS, d, 2 * tile), bf16),
                pltpu.VMEM((2, ff, q), bf16),
                pltpu.VMEM((m, ff), bf16),
                pltpu.VMEM((2, COLOURS, m, q), bf16),
                big, big, big, big,
                pltpu.VMEM((2, COLOURS, block, q), jnp.float32),
                small, small, small, small, small, small, small,
                dma, dma((SLOTS,)), dma((SLOTS,)), dma((2,)), dma((2, COLOURS)),
                dma((12, 2, COLOURS)), dma((12, 2, COLOURS)),
                pltpu.SemaphoreType.REGULAR((4,)),
            ],
            compiler_params=pltpu.CompilerParams(
                collective_id=0, has_side_effects=True, vmem_limit_bytes=66_000_000),
        )(x, w_gate, w_up, w_down)

    return jax.shard_map(
        body,
        mesh=mesh,
        in_specs=(P("dp", None), P(None, "tp"), P(None, "tp"), P("tp", None)),
        out_specs=P("dp", None),
        check_vma=False,
    )
```

```python
import functools
import math

import jax
import jax.numpy as jnp
from jax import lax
from jax.experimental import pallas as pl
from jax.experimental.pallas import tpu as pltpu
from jax.sharding import PartitionSpec as P

MESH = pl.DeviceIdType.MESH
COLOURS = 4
CHUNK = 256
TILE = 256
SLOTS = 3
R1, R2, R3, Q1, Q2, Q3, G1, G2, G3, H1, H2, H3 = range(12)


def kernel(cfg, x_hbm, wg_hbm, wu_hbm, wd_hbm, y_hbm,
           xb, wb, wdb, hb, term, r1, r2, r3, c3, run, s1, s2, q1, q2, q3, cq, fin,
           x_sem, wg_sem, wu_sem, wd_sem, own_sem, send_sem, recv_sem, credit):
    side, chunks, m, q, tiles, tile = cfg
    block, sub = m // side, m // (side * side)
    me = lax.axis_index("tp")
    px, py = me // side, me % side

    def dev(index):
        return {"tp": index}

    def place(k):
        ax = k // 2
        sign = 1 - 2 * (k % 2)
        p1, p2 = px * (1 - ax) + py * ax, py * (1 - ax) + px * ax
        return p1, p2, side * (1 - ax) + ax, (1 - ax) + side * ax, sign

    def step_on(p, stride, delta):
        return me + ((p + delta + side) % side - p) * stride

    def wrap(p, delta):
        return (p + delta + side) % side

    neighbours = [step_on(px, side, 1), step_on(px, side, -1), step_on(py, 1, 1), step_on(py, 1, -1)]
    def remote(kind, c, k, src, dst, to):
        return pltpu.make_async_remote_copy(
            src_ref=src, dst_ref=dst, send_sem=send_sem.at[kind, c % 2, k],
            recv_sem=recv_sem.at[kind, c % 2, k], device_id=dev(to), device_id_type=MESH)

    def rows_of(start, count):
        return pl.ds(pl.multiple_of(start, count), count)

    def y_at(c, k, p1, p2, count):
        return y_hbm.at[rows_of(c * m + p1 * block + p2 * sub, count), pl.ds(pl.multiple_of(k * q, 128), q)]

    def message(kind, c, k):
        p1, p2, st1, st2, s = place(k)
        par = c % 2
        plus1, minus1 = step_on(p1, st1, s), step_on(p1, st1, -s)
        plus2, minus2 = step_on(p2, st2, s), step_on(p2, st2, -s)
        if kind == R1:
            return remote(kind, c, k, term.at[par, k, rows_of(wrap(p1, 2) * block, block)], r1.at[par, k], minus1)
        if kind == R2:
            return remote(kind, c, k, term.at[par, k, rows_of(wrap(p1, s) * block, block)], r2.at[par, k], plus1)
        if kind == R3:
            return remote(kind, c, k, c3.at[par, k], r3.at[par, k], minus1)
        if kind == Q1:
            return remote(kind, c, k, s1.at[par, k], q1.at[par, k], minus2)
        if kind == Q2:
            return remote(kind, c, k, s2.at[par, k], q2.at[par, k], plus2)
        if kind == Q3:
            return remote(kind, c, k, cq.at[par, k], q3.at[par, k], minus2)
        if kind == G1:
            return remote(kind, c, k, fin.at[par, k], y_at(c, k, p1, p2, sub), plus2)
        if kind == G2:
            return remote(kind, c, k, fin.at[par, k], y_at(c, k, p1, p2, sub), minus2)
        if kind == G3:
            at = y_at(c, k, p1, wrap(p2, -s), sub)
            return remote(kind, c, k, at, at, plus2)
        if kind == H1:
            at = y_at(c, k, p1, 0, block)
            return remote(kind, c, k, at, at, plus1)
        if kind == H2:
            at = y_at(c, k, p1, 0, block)
            return remote(kind, c, k, at, at, minus1)
        at = y_at(c, k, wrap(p1, -s), 0, block)
        return remote(kind, c, k, at, at, plus1)

    def arrived(kind, c, k):
        p1, p2, _, _, s = place(k)
        par = c % 2
        dst = {
            R1: lambda: r1.at[par, k], R2: lambda: r2.at[par, k], R3: lambda: r3.at[par, k],
            Q1: lambda: q1.at[par, k], Q2: lambda: q2.at[par, k], Q3: lambda: q3.at[par, k],
            G1: lambda: y_at(c, k, p1, wrap(p2, -s), sub),
            G2: lambda: y_at(c, k, p1, wrap(p2, s), sub),
            G3: lambda: y_at(c, k, p1, wrap(p2, 2), sub),
            H1: lambda: y_at(c, k, wrap(p1, -s), 0, block),
            H2: lambda: y_at(c, k, wrap(p1, s), 0, block),
            H3: lambda: y_at(c, k, wrap(p1, 2), 0, block),
        }[kind]()
        pltpu.make_async_copy(dst, dst, recv_sem.at[kind, c % 2, k]).wait()

    def own_copy(c, k):
        p1, p2, _, _, _ = place(k)
        return pltpu.make_async_copy(fin.at[c % 2, k], y_at(c, k, p1, p2, sub), own_sem.at[c % 2, k])

    def colours(body):
        def one(k, carry):
            body(k, *place(k))
            return carry
        lax.fori_loop(0, COLOURS, one, 0)

    def by_rows(body):
        def one(i, carry):
            body(pl.multiple_of(i * sub, sub))
            return carry
        lax.fori_loop(0, side, one, 0)

    f32 = jnp.float32

    def stage1(c):
        par = c % 2

        def pass_on(k, p1, p2, st1, st2, s):
            message(R1, c, k).wait_send()
            arrived(R1, c, k)

            def add(i):
                at = pl.ds(i, sub)
                t = term[par, k, pl.ds(pl.multiple_of(wrap(p1, -s) * block + i, sub), sub), :]
                c3[par, k, at, :] = (t.astype(f32) + r1[par, k, at, :].astype(f32)).astype(jnp.bfloat16)
            by_rows(add)
            message(R3, c, k).start()

        def keep(k, p1, p2, st1, st2, s):
            message(R2, c, k).wait_send()
            arrived(R2, c, k)

            def add(i):
                at = pl.ds(i, sub)
                t = term[par, k, pl.ds(pl.multiple_of(p1 * block + i, sub), sub), :]
                run[par, k, at, :] = t.astype(f32) + r2[par, k, at, :].astype(f32)
            by_rows(add)
        colours(pass_on)
        colours(keep)

    def stage2(c):
        par = c % 2

        def body(k, p1, p2, st1, st2, s):
            message(R3, c, k).wait_send()
            arrived(R3, c, k)

            def add(i):
                at = pl.ds(i, sub)
                run[par, k, at, :] = run[par, k, at, :] + r3[par, k, at, :].astype(f32)
            by_rows(add)
            s1[par, k] = run[par, k, rows_of(wrap(p2, 2) * sub, sub), :].astype(jnp.bfloat16)
            s2[par, k] = run[par, k, rows_of(wrap(p2, s) * sub, sub), :].astype(jnp.bfloat16)
            message(Q1, c, k).start()
            message(Q2, c, k).start()
        colours(body)

    def stage3(c):
        par = c % 2

        def pass_on(k, p1, p2, st1, st2, s):
            message(Q1, c, k).wait_send()
            arrived(Q1, c, k)
            there = run[par, k, rows_of(wrap(p2, -s) * sub, sub), :]
            cq[par, k] = (there + q1[par, k].astype(f32)).astype(jnp.bfloat16)
            message(Q3, c, k).start()

        def keep(k, p1, p2, st1, st2, s):
            message(Q2, c, k).wait_send()
            arrived(Q2, c, k)
            mine = rows_of(p2 * sub, sub)
            run[par, k, mine, :] = run[par, k, mine, :] + q2[par, k].astype(f32)
        colours(pass_on)
        colours(keep)

    def stage4(c):
        par = c % 2

        def body(k, p1, p2, st1, st2, s):
            message(Q3, c, k).wait_send()
            arrived(Q3, c, k)
            mine = rows_of(p2 * sub, sub)
            fin[par, k] = (run[par, k, mine, :] + q3[par, k].astype(f32)).astype(jnp.bfloat16)
            message(G1, c, k).start()
            own_copy(c, k).start()
        colours(body)
        colours(lambda k, *_: message(G2, c, k).start())

    def stage5(c):
        def pass_on(k, *_):
            message(G1, c, k).wait_send()
            arrived(G1, c, k)
            message(G3, c, k).start()

        def rest(k, *_):
            message(G2, c, k).wait_send()
            own_copy(c, k).wait()
            arrived(G2, c, k)
        colours(pass_on)
        colours(rest)

    def stage6(c):
        def body(k, *_):
            message(G3, c, k).wait_send()
            arrived(G3, c, k)
            message(H1, c, k).start()
        colours(body)
        colours(lambda k, *_: message(H2, c, k).start())

    def stage7(c):
        def pass_on(k, *_):
            message(H1, c, k).wait_send()
            arrived(H1, c, k)
            message(H3, c, k).start()

        def rest(k, *_):
            message(H2, c, k).wait_send()
            arrived(H2, c, k)
        colours(pass_on)
        colours(rest)

    def stage8(c):
        def body(k, *_):
            message(H3, c, k).wait_send()
            arrived(H3, c, k)
        colours(body)

    def x_copy(t):
        return pltpu.make_async_copy(x_hbm.at[rows_of(t * m, m), :], xb, x_sem)

    def w_copies(g):
        at = pl.ds(pl.multiple_of((g % tiles) * tile, tile), tile)
        slot = g % SLOTS
        return (pltpu.make_async_copy(wg_hbm.at[:, at], wb.at[slot, :, pl.ds(0, tile)], wg_sem.at[slot]),
                pltpu.make_async_copy(wu_hbm.at[:, at], wb.at[slot, :, pl.ds(tile, tile)], wu_sem.at[slot]))

    def colour_at(j):
        return (j % 2) * 2 + j // 2

    def d_copy(j):
        at = pl.ds(pl.multiple_of(colour_at(j) * q, 128), q)
        return pltpu.make_async_copy(wd_hbm.at[:, at], wdb.at[j % 2], wd_sem.at[j % 2])

    x_copy(0).start()
    for g in range(SLOTS):
        for copy in w_copies(g):
            copy.start()

    barrier = pltpu.get_barrier_semaphore()
    for other in neighbours:
        pl.semaphore_signal(barrier, inc=1, device_id=dev(other), device_id_type=MESH)
    pl.semaphore_wait(barrier, len(neighbours))

    def hidden(t, n):
        @pl.when(n == 0)
        def _():
            x_copy(t).wait()
        g = t * tiles + n
        slot = g % SLOTS
        for copy in w_copies(g):
            copy.wait()
        both = jnp.dot(xb[...], wb[slot], preferred_element_type=f32)
        gate, up = both[:, :tile], both[:, tile:]
        at = pl.ds(pl.multiple_of(n * tile, tile), tile)
        hb[:, at] = (gate * jax.nn.sigmoid(gate) * up).astype(jnp.bfloat16)

        @pl.when(g + SLOTS < chunks * tiles)
        def _():
            for copy in w_copies(g + SLOTS):
                copy.start()

        @pl.when((t == 0) & (n >= tiles - 2))
        def _():
            d_copy(n - (tiles - 2)).start()

        @pl.when((n == tiles - 1) & (t + 1 < chunks))
        def _():
            x_copy(t + 1).start()

    def down(t, j):
        k = colour_at(j)
        d_copy(j).wait()
        term[t % 2, k] = jnp.dot(hb[...], wdb[j % 2], preferred_element_type=f32).astype(jnp.bfloat16)
        message(R1, t, k).start()
        message(R2, t, k).start()

        @pl.when((j + 2 < COLOURS) | (t + 1 < chunks))
        def _():
            d_copy((j + 2) % COLOURS).start()

    steps = chunks + 5

    def handle(t, *stages):
        for lag, stage in stages:
            @pl.when((t >= lag) & (t < chunks + lag))
            def _(stage=stage, lag=lag):
                stage(t - lag)

    def at_tile(n, late):
        return n == max(tiles - 1 - late, 0)

    def step(t, carry):
        @pl.when(t > 0)
        def _():
            for d in range(len(neighbours)):
                pl.semaphore_wait(credit.at[d], 1)

        def tile_step(n, carry):
            @pl.when(t < chunks)
            def _():
                hidden(t, n)

            @pl.when(at_tile(n, 4))
            def _():
                handle(t, (5, stage7))

            @pl.when(at_tile(n, 3))
            def _():
                handle(t, (2, stage3), (3, stage5))

            @pl.when(at_tile(n, 2))
            def _():
                handle(t, (1, stage1), (4, stage6))

            @pl.when(at_tile(n, 1))
            def _():
                handle(t, (2, stage4), (5, stage8))
            return carry
        lax.fori_loop(0, tiles, tile_step, 0)

        @pl.when(t < steps - 1)
        def _():
            for d, other in enumerate(neighbours):
                pl.semaphore_signal(credit.at[d], inc=1, device_id=dev(other), device_id_type=MESH)

        handle(t, (1, stage2))

        def colour_step(j, carry):
            @pl.when(t < chunks)
            def _():
                down(t, j)
            return carry
        lax.fori_loop(0, COLOURS, colour_step, 0)
        return carry

    lax.fori_loop(0, steps, step, 0)


def solution(mesh):
    side = math.isqrt(mesh.shape["tp"])
    assert side == 4 and side * side == mesh.shape["tp"]

    def body(x, w_gate, w_up, w_down):
        rows, d = x.shape
        ff = w_gate.shape[1]
        m, q, tile = CHUNK, d // COLOURS, TILE
        chunks, tiles = rows // m, ff // tile
        block, sub = m // side, m // (side * side)
        bf16 = jnp.bfloat16
        any_spec = pl.BlockSpec(memory_space=pl.ANY)
        dma = pltpu.SemaphoreType.DMA
        big = pltpu.VMEM((2, COLOURS, block, q), bf16)
        small = pltpu.VMEM((2, COLOURS, sub, q), bf16)
        return pl.pallas_call(
            functools.partial(kernel, (side, chunks, m, q, tiles, tile)),
            out_shape=jax.ShapeDtypeStruct((rows, d), bf16),
            in_specs=[any_spec] * 4,
            out_specs=any_spec,
            scratch_shapes=[
                pltpu.VMEM((m, d), bf16),
                pltpu.VMEM((SLOTS, d, 2 * tile), bf16),
                pltpu.VMEM((2, ff, q), bf16),
                pltpu.VMEM((m, ff), bf16),
                pltpu.VMEM((2, COLOURS, m, q), bf16),
                big, big, big, big,
                pltpu.VMEM((2, COLOURS, block, q), jnp.float32),
                small, small, small, small, small, small, small,
                dma, dma((SLOTS,)), dma((SLOTS,)), dma((2,)), dma((2, COLOURS)),
                dma((12, 2, COLOURS)), dma((12, 2, COLOURS)),
                pltpu.SemaphoreType.REGULAR((4,)),
            ],
            compiler_params=pltpu.CompilerParams(
                collective_id=0, has_side_effects=True, vmem_limit_bytes=66_000_000),
        )(x, w_gate, w_up, w_down)

    return jax.shard_map(
        body,
        mesh=mesh,
        in_specs=(P("dp", None), P(None, "tp"), P(None, "tp"), P("tp", None)),
        out_specs=P("dp", None),
        check_vma=False,
    )
```
